32 devices in a mesh: pop: 4 (over x, core), tp: 4 (over z), pp: 2 (over y).
Axes of the slice: x: 2, y: 2, z: 4, core: 2. Of those that a mesh axis runs over, the one named last changes fastest.
Arguments:
- hidden_in: bfloat16 [256, 8, 4096], P('tp', 'pop'), may hold values from -6 to 6
- norm_gain: float32 [2, 4096], P('pp'), may hold values from 0.5 to 1.5
- w_gate: bfloat16 [2, 4096, 12288], P('pp', None, 'tp'), may hold values from -0.09375 to 0.09375
- w_up: bfloat16 [2, 4096, 12288], P('pp', None, 'tp'), may hold values from -0.09375 to 0.09375
- w_down: bfloat16 [2, 12288, 4096], P('pp', 'tp'), may hold values from -0.0546875 to 0.0546875
- gate_left: bfloat16 [2, 8, 4096], P('pp', 'pop'), may hold values from -6 to 6
- gate_right: bfloat16 [2, 8, 12288], P('pp', 'pop', 'tp'), may hold values from -6 to 6
- up_left: bfloat16 [2, 8, 4096], P('pp', 'pop'), may hold values from -6 to 6
- up_right: bfloat16 [2, 8, 12288], P('pp', 'pop', 'tp'), may hold values from -6 to 6
- down_left: bfloat16 [2, 8, 12288], P('pp', 'pop', 'tp'), may hold values from -6 to 6
- down_right: bfloat16 [2, 8, 4096], P('pp', 'pop'), may hold values from -6 to 6
- ranks: int32 [8], P('pop'), may hold values from 0 to 7, each once
Outputs:
- section_out: bfloat16 [2, 256, 8, 4096], P('pp', 'tp', 'pop')
- update_gate: bfloat16 [2, 4096, 12288], P('pp', 'pop', 'tp')
- update_up: bfloat16 [2, 4096, 12288], P('pp', 'pop', 'tp')
- update_down: bfloat16 [2, 12288, 4096], P('pp', 'tp', 'pop')
The draws below stay inside these ranges and needn't reach their ends.
Inputs may be any that keep to these rules, and one draw needn't show every extreme that they name: `ranks`: each number from 0 to 7 is the rank of exactly one member.
All inputs are finite; a program needn't handle non-finite values.
Results may differ from the reference program's by a relative error of at most 0.014.
Values may be sent and summed in bfloat16 or wider, within the bound.
A program may use at most 256 MiB of HBM per device.

```python
import math
import jax
import jax.numpy as jnp
from jax import lax

D = 4096
FF = 12288
SEQ = 256
MEM_DEV = 2
POP = 8
SECTIONS = 2
N_POP = 4


def shard_levels(key, shape, split, low, high):
    loudness, own = 1.0, jax.random.fold_in(key, 6)
    for axis_at, parts in split:
        draws = jnp.exp(jax.random.uniform(jax.random.fold_in(own, axis_at), (parts,), jnp.float32, low / len(split), high / len(split)))
        loudness = loudness * jnp.repeat(draws, shape[axis_at] // parts).reshape([-1 if axis == axis_at else 1 for axis in range(len(shape))])
    return loudness


def normal_values(rng, shape, deviation, most, pieces=(), held_as=jnp.bfloat16):
    array = jax.random.normal(rng, shape, jnp.float32) * deviation
    if len(pieces) > 0:
        array = shard_levels(rng, shape, pieces, -0.22, 0.18) * array
    return jnp.clip(array, min=-most, max=most).astype(held_as)


def setup_inputs(seed: int = 0) -> dict:
    streams_of = jax.random.split(jax.random.key(seed), 13)
    hidden_in = normal_values(streams_of[0], (SEQ, POP, D), 1.0, 6.0, ((0, 4), (1, 4)))
    norm_gain = jnp.clip(1.0 + 0.1 * jax.random.normal(streams_of[1], (SECTIONS, D), jnp.float32), 0.5, 1.5)
    w_gate = normal_values(streams_of[2], (SECTIONS, D, FF), D ** -0.5, 0.09375, ((0, 2), (2, 4)))
    w_up = normal_values(streams_of[3], (SECTIONS, D, FF), D ** -0.5, 0.09375, ((0, 2), (2, 4)))
    w_down = normal_values(streams_of[4], (SECTIONS, FF, D), FF ** -0.5, 0.0546875, ((0, 2), (1, 4)))
    gate_left = normal_values(streams_of[5], (SECTIONS, POP, D), 1.0, 6.0, ((0, 2), (1, 4)))
    gate_right = normal_values(streams_of[6], (SECTIONS, POP, FF), 1.0, 6.0, ((0, 2), (1, 4), (2, 4)))
    up_left = normal_values(streams_of[7], (SECTIONS, POP, D), 1.0, 6.0, ((0, 2), (1, 4)))
    up_right = normal_values(streams_of[8], (SECTIONS, POP, FF), 1.0, 6.0, ((0, 2), (1, 4), (2, 4)))
    down_left = normal_values(streams_of[9], (SECTIONS, POP, FF), 1.0, 6.0, ((0, 2), (1, 4), (2, 4)))
    down_right = normal_values(streams_of[10], (SECTIONS, POP, D), 1.0, 6.0, ((0, 2), (1, 4)))
    ranks = jax.random.permutation(streams_of[11], POP).astype(jnp.int32)
    return {"hidden_in": hidden_in, "norm_gain": norm_gain, "w_gate": w_gate, "w_up": w_up, "w_down": w_down, "gate_left": gate_left, "gate_right": gate_right, "up_left": up_left, "up_right": up_right, "down_left": down_left, "down_right": down_right, "ranks": ranks}


sigma_scale = 0.3
norm_eps = 1e-05

def section_layer(hidden, gain, w_gate, w_up, w_down, gate_left, gate_right, up_left, up_right, down_left, down_right):
    values = hidden.astype(jnp.float32)
    mean_sq = lax.optimization_barrier(jnp.mean(values * values, axis=-1, keepdims=True))
    normed = (values * lax.rsqrt(mean_sq + norm_eps) * gain).astype(jnp.bfloat16)
    flat = normed.reshape(SEQ * POP, D)
    normed_wide = normed.astype(jnp.float32)
    coef_in = sigma_scale / math.sqrt(D)
    coef_hidden = sigma_scale / math.sqrt(FF)
    gate = jnp.dot(flat, w_gate, preferred_element_type=jnp.float32).reshape(SEQ, POP, FF)
    gate_side = jnp.einsum('spd,pd->sp', normed_wide, gate_left.astype(jnp.float32))
    gate = gate + coef_in * gate_side[:, :, None] * gate_right.astype(jnp.float32)[None]
    upper = jnp.dot(flat, w_up, preferred_element_type=jnp.float32).reshape(SEQ, POP, FF)
    up_side = jnp.einsum('spd,pd->sp', normed_wide, up_left.astype(jnp.float32))
    upper = upper + coef_in * up_side[:, :, None] * up_right.astype(jnp.float32)[None]
    inner = (jax.nn.silu(gate) * upper).astype(jnp.bfloat16)
    term = jnp.dot(inner.reshape(SEQ * POP, FF), w_down, preferred_element_type=jnp.float32).reshape(SEQ, POP, D)
    down_side = jnp.einsum('spf,pf->sp', inner.astype(jnp.float32), down_left.astype(jnp.float32))
    term = term + coef_hidden * down_side[:, :, None] * down_right.astype(jnp.float32)[None]
    return (values + term).astype(jnp.bfloat16)

def grouped_outer(fitness, left, right):
    total = jnp.zeros((left.shape[1], right.shape[1]), jnp.float32)
    for group in range(N_POP):
        lower = group * MEM_DEV
        weighted = fitness[lower:lower + MEM_DEV, None] * left[lower:lower + MEM_DEV].astype(jnp.float32)
        part = jnp.dot(weighted.T, right[lower:lower + MEM_DEV].astype(jnp.float32), precision=lax.Precision.HIGHEST)
        total = total + lax.optimization_barrier(part.astype(jnp.bfloat16)).astype(jnp.float32)
    return total.astype(jnp.bfloat16)

def reference(hidden_in, norm_gain, w_gate, w_up, w_down, gate_left, gate_right, up_left, up_right, down_left, down_right, ranks):
    current = hidden_in
    outputs = []
    for section in range(SECTIONS):
        current = section_layer(current, norm_gain[section], w_gate[section], w_up[section], w_down[section], gate_left[section], gate_right[section], up_left[section], up_right[section], down_left[section], down_right[section])
        outputs.append(current)
    section_out = jnp.stack(outputs)
    fitness = (2.0 * ranks.astype(jnp.float32) / (POP - 1) - 1.0) / math.sqrt(POP)
    update_gate = jnp.stack([grouped_outer(fitness, gate_left[section], gate_right[section]) for section in range(SECTIONS)])
    update_up = jnp.stack([grouped_outer(fitness, up_left[section], up_right[section]) for section in range(SECTIONS)])
    update_down = jnp.stack([grouped_outer(fitness, down_left[section], down_right[section]) for section in range(SECTIONS)])
    return (section_out, update_gate, update_up, update_down)
```

```python
import functools
import math

import jax
import jax.numpy as jnp
from jax import lax
from jax.experimental import pallas as pl
from jax.experimental.pallas import tpu as pltpu
from jax.sharding import PartitionSpec as P

MESH = pl.DeviceIdType.MESH
f32, bf16 = jnp.float32, jnp.bfloat16

sigma_scale = 0.3
norm_eps = 1e-05

ROWS = 32
HOP_TICKS = 4
GATHER_TICKS = 4
VMEM_BYTES = 66_000_000


def widths(D, F):
    hidden = next(w for w in (256, 128) if F % w == 0)
    columns = next(w for w in (512, 256, 128) if D % w == 0 and D // w >= 4)
    return hidden, columns


def relay_kernel(
    dims,
    x_hbm, wg_hbm, wu_hbm, wd_hbm, gain, lefts, gr, ur, dl, dr, vec,
    out_hbm, every_hbm,
    xh, nb, hid, part, rr, ll, xo, acc, side_g, side_u, side_d, wg, wu, wd, ve,
    w_sem, wd_sem, hop_recv, hop_send, out_sem,
    ag_recv, ag_right, ag_left, rr_recv, rr_send, ll_recv, ll_send,
    v_send, v_recv, v_out,
):
    n, T, S, Pn, members, D, F, HB, DB, keep, ring, dring = dims
    J, Nd, M = F // HB, D // DB, T * ROWS
    me, s, p = lax.axis_index("tp"), lax.axis_index("pp"), lax.axis_index("pop")
    coef_in = sigma_scale / math.sqrt(D)
    coef_hidden = sigma_scale / math.sqrt(F * T)
    has_left, has_right = me > 0, me < T - 1
    has_prev, has_next = s > 0, s < S - 1
    stream = J - keep

    def gu_copies(j, slot):
        cols = pl.ds(pl.multiple_of(j * HB, HB), HB)
        return (
            pltpu.make_async_copy(wg_hbm.at[:, cols], wg.at[slot], w_sem.at[slot, 0]),
            pltpu.make_async_copy(wu_hbm.at[:, cols], wu.at[slot], w_sem.at[slot, 1]),
        )

    def wd_copy(b, slot):
        cols = pl.ds(pl.multiple_of(b * DB, DB), DB)
        return pltpu.make_async_copy(wd_hbm.at[:, cols], wd.at[slot], wd_sem.at[slot])

    def start(copies):
        for copy in copies:
            copy.start()

    def own_copy(c, b):
        cols = pl.ds(pl.multiple_of(b * DB, DB), DB)
        return pltpu.make_async_copy(x_hbm.at[c, :, cols], xh.at[c, :, cols], hop_recv.at[c, b])

    def each(count, body):
        lax.fori_loop(0, count, lambda i, z: (body(i), z)[1], 0)

    def between(lo, hi, body):
        lax.fori_loop(lo, hi, lambda i, z: (body(i), z)[1], 0)

    @pl.when(s == 0)
    def _():
        each(n, lambda c: each(Nd, lambda b: own_copy(c, b).start()))

    for j in range(keep + ring):
        start(gu_copies(j, j))
    for b in range(dring):
        wd_copy(b, b).start()

    barrier = pltpu.get_barrier_semaphore()

    def greet(cond, device):
        @pl.when(cond)
        def _():
            pl.semaphore_signal(barrier, inc=1, device_id=device, device_id_type=MESH)

    greet(has_left, {"tp": me - 1})
    greet(has_right, {"tp": me + 1})
    greet(has_prev, {"pp": s - 1})
    greet(has_next, {"pp": s + 1})
    for k in range(1, Pn):
        pl.semaphore_signal(barrier, inc=1, device_id={"pop": lax.rem(p + k, Pn)}, device_id_type=MESH)
    as_int = lambda v: v.astype(jnp.int32)
    pl.semaphore_wait(barrier, as_int(has_left) + as_int(has_right) + as_int(has_prev) + as_int(has_next) + Pn - 1)

    def vec_copy(k):
        return pltpu.make_async_remote_copy(
            src_ref=vec, dst_ref=ve.at[k - 1], send_sem=v_send.at[k - 1], recv_sem=v_recv.at[k - 1],
            device_id={"pop": lax.rem(p + k, Pn)}, device_id_type=MESH,
        )

    def ag_copy(c, o, right):
        return pltpu.make_async_remote_copy(
            src_ref=nb.at[c, o], dst_ref=nb.at[c, o],
            send_sem=(ag_right if right else ag_left).at[c, o], recv_sem=ag_recv.at[c, o],
            device_id={"tp": me + 1 if right else me - 1}, device_id_type=MESH,
        )

    def ag_send(c, o, cond, right):
        @pl.when(cond)
        def _():
            ag_copy(c, o, right).start()

    def normalize(c):
        total = jnp.zeros((ROWS, 1), f32)
        for b in range(Nd):
            own_copy(c, b).wait()
            values = xh[c, :, b * DB : (b + 1) * DB].astype(f32)
            total = total + jnp.sum(values * values, axis=-1, keepdims=True)
        scale = lax.rsqrt(total / D + norm_eps)
        for b in range(Nd):
            cols = slice(b * DB, (b + 1) * DB)
            values = xh[c, :, cols].astype(f32)
            nb[c, me, :, cols] = (values * scale * gain[:, cols]).astype(bf16)
        ag_send(c, me, has_right, True)
        ag_send(c, me, has_left, False)

    def ag_step(c, k):
        @pl.when(k == 0)
        def _():
            normalize(c)

        @pl.when(jnp.logical_and(k > 0, me - k >= 0))
        def _():
            o = me - k
            ag_copy(c, o, True).wait_recv()
            ag_send(c, o, has_right, True)

        @pl.when(jnp.logical_and(k > 0, me + k < T))
        def _():
            o = me + k
            ag_copy(c, o, False).wait_recv()
            ag_send(c, o, has_left, False)

    def sum_copy(c, b, o, right):
        buf = rr if right else ll
        return pltpu.make_async_remote_copy(
            src_ref=buf.at[c, b, o], dst_ref=buf.at[c, b, o],
            send_sem=(rr_send if right else ll_send).at[c, b, o],
            recv_sem=(rr_recv if right else ll_recv).at[c, b, o],
            device_id={"tp": me + 1 if right else me - 1}, device_id_type=MESH,
        )

    def pass_on(c, b, right):
        buf = rr if right else ll
        first = jnp.logical_not(has_left if right else has_right)

        def one(o):
            @pl.when(first)
            def _():
                buf[c, b, o] = part[b, o]

            @pl.when(jnp.logical_not(first))
            def _():
                sum_copy(c, b, o, right).wait_recv()
                buf[c, b, o] = (buf[c, b, o].astype(f32) + part[b, o].astype(f32)).astype(bf16)

            sum_copy(c, b, o, right).start()

        if right:
            between(me + 1, T, one)
        else:
            between(0, me, one)

    def hop_copy(c, b):
        cols = pl.ds(pl.multiple_of(b * DB, DB), DB)
        return pltpu.make_async_remote_copy(
            src_ref=xo.at[c, :, cols], dst_ref=xh.at[c, :, cols],
            send_sem=hop_send.at[c, b], recv_sem=hop_recv.at[c, b],
            device_id={"pp": s + 1}, device_id_type=MESH,
        )

    def out_copy(c, b):
        cols = pl.ds(pl.multiple_of(b * DB, DB), DB)
        return pltpu.make_async_copy(xo.at[c, :, cols], out_hbm.at[c, :, cols], out_sem.at[c, b])

    def finish(c, b):
        cols = pl.ds(pl.multiple_of(b * DB, DB), DB)
        acc[...] = part[b, me].astype(f32)

        @pl.when(has_left)
        def _():
            sum_copy(c, b, me, True).wait_recv()
            acc[...] += rr[c, b, me].astype(f32)

        @pl.when(has_right)
        def _():
            sum_copy(c, b, me, False).wait_recv()
            acc[...] += ll[c, b, me].astype(f32)

        xo[c, :, cols] = (xh[c, :, cols].astype(f32) + acc[...]).astype(bf16)
        out_copy(c, b).start()

        @pl.when(has_next)
        def _():
            hop_copy(c, b).start()

    last_hop = jnp.maximum(me, T - 1 - me)

    def rs_step(c, i):
        def at(lag, body):
            b = i - lag * HOP_TICKS

            @pl.when(jnp.logical_and(b >= 0, b < Nd))
            def _():
                body(b)

        at(me, lambda b: pass_on(c, b, True))
        at(T - 1 - me, lambda b: pass_on(c, b, False))
        at(last_hop, lambda b: finish(c, b))

    rs_steps = Nd + (T - 1) * HOP_TICKS
    spill = -(-(rs_steps - Nd) // J)

    ticks = J + Nd
    begin = jnp.where(s == 0, 1, 8)

    def gathered(tick):
        done = jnp.clip((tick - begin + GATHER_TICKS) // GATHER_TICKS, 0, T)
        return jnp.where(tick >= ticks - 1, T, done)

    def communicate(c, tick):
        @pl.when(c + 1 < n)
        def _():
            lo = jnp.where(tick == 0, 0, gathered(tick - 1))
            between(lo, gathered(tick), lambda k: ag_step(c + 1, k))

    def member_side(sides, first):
        member = lax.broadcasted_iota(jnp.int32, sides.shape, 0) % members + first
        column = lax.broadcasted_iota(jnp.int32, sides.shape, 1)
        return jnp.sum(jnp.where(member == column, sides, 0.0), axis=1, keepdims=True)

    def add_side(product, side, right):
        wide = product.reshape(T, ROWS, product.shape[-1])
        wide = wide + side[...].reshape(T, ROWS, 1) * right.astype(f32)[None]
        return wide.reshape(product.shape)

    NT = (((1,), (1,)), ((), ()))

    each(T, lambda k: ag_step(0, k))
    for k in range(1, Pn):
        vec_copy(k).start()

    def chunk(c):
        rows = lambda: nb[c].reshape(M, D)
        sides = coef_in * lax.dot_general(rows(), lefts[...], NT, preferred_element_type=f32)
        side_g[...] = member_side(sides, 0)
        side_u[...] = member_side(sides, members)

        def gu(j):
            if stream:
                q = c * stream + j - keep
                slot = jnp.where(j < keep, j, keep + (q + ring) % ring)
            else:
                q, slot = 0, j

            @pl.when(jnp.logical_or(c == 0, j >= keep))
            def _():
                for copy in gu_copies(j, slot):
                    copy.wait()

            cols = pl.ds(pl.multiple_of(j * HB, HB), HB)
            x = rows()
            gate = jnp.dot(x, wg[slot], preferred_element_type=f32)
            upper = jnp.dot(x, wu[slot], preferred_element_type=f32)
            gate = add_side(gate, side_g, gr[:, cols])
            upper = add_side(upper, side_u, ur[:, cols])
            hid[:, cols] = (gate / (1.0 + jnp.exp(-gate)) * upper).astype(bf16)
            if stream:
                ahead = q + ring

                @pl.when(jnp.logical_and(j >= keep, ahead < n * stream))
                def _():
                    start(gu_copies(keep + ahead % stream, slot))

            @pl.when(c > 0)
            def _():
                between(Nd + j * spill, jnp.minimum(Nd + (j + 1) * spill, rs_steps), lambda i: rs_step(c - 1, i))

            communicate(c, j)

        each(J, gu)
        side_d[...] = member_side(coef_hidden * lax.dot_general(hid[...], dl[...], NT, preferred_element_type=f32), 0)

        def down(b):
            q = c * Nd + b
            slot = q % dring
            cols = pl.ds(pl.multiple_of(b * DB, DB), DB)
            wd_copy(b, slot).wait()
            term = jnp.dot(hid[...], wd[slot], preferred_element_type=f32)
            part[b] = add_side(term, side_d, dr[:, cols]).astype(bf16).reshape(T, ROWS, DB)

            @pl.when(q + dring < n * Nd)
            def _():
                wd_copy((b + dring) % Nd, slot).start()

            rs_step(c, b)
            communicate(c, J + b)

        each(Nd, down)

    each(n, chunk)
    between(Nd, rs_steps, lambda i: rs_step(n - 1, i))

    out_own = pltpu.make_async_copy(vec, every_hbm.at[p], v_out.at[Pn - 1])
    out_own.start()
    for k in range(1, Pn):
        vec_copy(k).wait()
        pltpu.make_async_copy(ve.at[k - 1], every_hbm.at[lax.rem(p + Pn - k, Pn)], v_out.at[k - 1]).start()

    def drain(c):
        def gather(o):
            @pl.when(jnp.logical_and(has_right, o <= me))
            def _():
                ag_copy(c, o, True).wait_send()

            @pl.when(jnp.logical_and(has_left, o >= me))
            def _():
                ag_copy(c, o, False).wait_send()

        each(T, gather)

        def block(b):
            between(me + 1, T, lambda o: sum_copy(c, b, o, True).wait_send())
            between(0, me, lambda o: sum_copy(c, b, o, False).wait_send())
            out_copy(c, b).wait()

            @pl.when(has_next)
            def _():
                hop_copy(c, b).wait_send()

        each(Nd, block)

    each(n, drain)
    out_own.wait()
    for k in range(1, Pn):
        pltpu.make_async_copy(ve.at[k - 1], every_hbm.at[lax.rem(p + Pn - k, Pn)], v_out.at[k - 1]).wait()


def relay(x, w_gate, w_up, w_down, gain, lefts, gr, ur, dl, dr, vec, members):
    n, _, D = x.shape
    F = w_gate.shape[1]
    T, S, Pn = (lax.axis_size(a) for a in ("tp", "pp", "pop"))
    HB, DB = widths(D, F)
    J, Nd, M = F // HB, D // DB, T * ROWS
    dring = min(3, Nd)
    fixed = 2 * (3 * n * ROWS * D + n * M * D + M * F + M * D + 2 * n * M * D + dring * F * DB) + 6_000_000
    slots = min(J, (VMEM_BYTES - fixed) // (4 * D * HB))
    ring = 0 if slots == J else min(3, slots)
    keep = slots - ring
    dims = (n, T, S, Pn, members, D, F, HB, DB, keep, ring, dring)
    vmem, hbm = pl.BlockSpec(memory_space=pltpu.VMEM), pl.BlockSpec(memory_space=pl.ANY)
    dma = pltpu.SemaphoreType.DMA
    return pl.pallas_call(
        functools.partial(relay_kernel, dims),
        out_shape=(
            jax.ShapeDtypeStruct((n, ROWS, D), bf16),
            jax.ShapeDtypeStruct((Pn,) + vec.shape, bf16),
        ),
        in_specs=[hbm] * 4 + [vmem] * 7,
        out_specs=(hbm, hbm),
        scratch_shapes=[
            pltpu.VMEM((n, ROWS, D), bf16),
            pltpu.VMEM((n, T, ROWS, D), bf16),
            pltpu.VMEM((M, F), bf16),
            pltpu.VMEM((Nd, T, ROWS, DB), bf16),
            pltpu.VMEM((n, Nd, T, ROWS, DB), bf16),
            pltpu.VMEM((n, Nd, T, ROWS, DB), bf16),
            pltpu.VMEM((n, ROWS, D), bf16),
            pltpu.VMEM((ROWS, DB), f32),
            pltpu.VMEM((M, 1), f32),
            pltpu.VMEM((M, 1), f32),
            pltpu.VMEM((M, 1), f32),
            pltpu.VMEM((slots, D, HB), bf16),
            pltpu.VMEM((slots, D, HB), bf16),
            pltpu.VMEM((dring, F, DB), bf16),
            pltpu.VMEM((Pn - 1,) + vec.shape, bf16),
            dma((slots, 2)),
            dma((dring,)),
            dma((n, Nd)),
            dma((n, Nd)),
            dma((n, Nd)),
            dma((n, T)),
            dma((n, T)),
            dma((n, T)),
            dma((n, Nd, T)),
            dma((n, Nd, T)),
            dma((n, Nd, T)),
            dma((n, Nd, T)),
            dma((Pn - 1,)),
            dma((Pn - 1,)),
            dma((Pn,)),
        ],
        compiler_params=pltpu.CompilerParams(collective_id=0, has_side_effects=True, vmem_limit_bytes=67_000_000),
    )(x, w_gate, w_up, w_down, gain, lefts, gr, ur, dl, dr, vec)


def low_rank(left, right, fitness):
    weighted = fitness[:, None] * left.astype(f32)
    high = lax.reduce_precision(weighted, 8, 7)
    both = jnp.concatenate([high, weighted - high]).astype(bf16)
    return jnp.einsum("pi,pj->ij", both, jnp.concatenate([right, right]), preferred_element_type=f32).astype(bf16)


def per_device(
    hidden_in, norm_gain, w_gate, w_up, w_down,
    gate_left, gate_right, up_left, up_right, down_left, down_right, ranks,
):
    tokens, members, D = hidden_in.shape
    F = w_gate.shape[2]
    Pn = lax.axis_size("pop")
    n = tokens * members // ROWS
    x = hidden_in.reshape(n, ROWS, D)

    def rows16(*vectors):
        stacked = jnp.concatenate(vectors)
        return jnp.pad(stacked, ((0, -stacked.shape[0] % 16), (0, 0)))

    def expand(vectors):
        return jnp.tile(vectors, (ROWS // members, 1))

    vectors = [gate_left[0], gate_right[0], up_left[0], up_right[0], down_left[0], down_right[0]]
    column = jnp.broadcast_to(ranks.astype(bf16)[:, None], (members, 128))
    pieces = [v.reshape(-1, 128) for v in vectors + [column]]
    lengths = [piece.shape[0] for piece in pieces]
    packed = rows16(*pieces)

    out, everyone = relay(
        x, w_gate[0], w_up[0], w_down[0], norm_gain,
        rows16(gate_left[0], up_left[0]), expand(gate_right[0]), expand(up_right[0]),
        rows16(down_left[0]), expand(down_right[0]), packed, members,
    )

    population = members * Pn
    ends = [sum(lengths[: i + 1]) for i in range(len(lengths))]
    gl, gr, ul, ur, dl, dr, rank = [
        everyone[:, end - length : end].reshape(population, -1) for end, length in zip(ends, lengths)
    ]
    fitness = (2.0 * rank[:, 0].astype(f32) / (population - 1) - 1.0) / math.sqrt(population)
    share_size = D // Pn
    first = lax.axis_index("pop") * share_size

    def share(full):
        return lax.dynamic_slice_in_dim(full, first, share_size, 1)

    return (
        out.reshape(1, tokens, members, D),
        low_rank(share(gl), gr, fitness)[None],
        low_rank(share(ul), ur, fitness)[None],
        low_rank(dl, share(dr), fitness)[None],
    )


def solution(mesh):
    placed = (
        P("tp", "pop", None),
        P("pp", None),
        P("pp", None, "tp"),
        P("pp", None, "tp"),
        P("pp", "tp", None),
        P("pp", "pop", None),
        P("pp", "pop", "tp"),
        P("pp", "pop", None),
        P("pp", "pop", "tp"),
        P("pp", "pop", "tp"),
        P("pp", "pop", None),
        P("pop"),
    )
    return jax.shard_map(
        per_device,
        mesh=mesh,
        in_specs=placed,
        out_specs=(
            P("pp", "tp", "pop", None),
            P("pp", "pop", "tp"),
            P("pp", "pop", "tp"),
            P("pp", "tp", "pop"),
        ),
        check_vma=False,
    )
```

```python
import functools
import math

import jax
import jax.numpy as jnp
from jax import lax
from jax.experimental import pallas as pl
from jax.experimental.pallas import tpu as pltpu
from jax.sharding import PartitionSpec as P

MESH = pl.DeviceIdType.MESH
f32, bf16 = jnp.float32, jnp.bfloat16

sigma_scale = 0.3
norm_eps = 1e-05

ROWS = 32
HOP_TICKS = 4
GATHER_TICKS = 2
FIRST_BEGIN = 1
LATER_BEGIN = 3
VMEM_BYTES = 66_000_000
RESERVE = 1_500_000


def widths(D, F):
    hidden = next(w for w in (256, 128) if F % w == 0)
    columns = next(w for w in (512, 256, 128) if D % w == 0 and D // w >= 4)
    return hidden, columns


def relay_kernel(
    dims,
    x_hbm, wg_hbm, wu_hbm, wd_hbm, gain, gl, gr, ul, ur, dl, dr, fit, token,
    out_hbm, egl, egr, eul, eur, edl, edr, efit,
    gx, xn, hid, part, rr, ll, xo, acc, side_g, side_u, side_d, wg, wu, wd, stack, lefts, downs,
    w_sem, wd_sem, hop_recv, hop_send, out_sem,
    ag_recv, ag_right, ag_left, rr_recv, rr_send, ll_recv, ll_send,
    v_send, v_recv, v_own, ready,
):
    n, T, S, Pn, members, D, F, HB, DB, keep, ring, dring = dims
    J, Nd, M = F // HB, D // DB, T * ROWS
    G = Nd // 2 if Nd % 2 == 0 else Nd
    GW = D // G
    me, s, p = lax.axis_index("tp"), lax.axis_index("pp"), lax.axis_index("pop")
    coef_in = sigma_scale / math.sqrt(D)
    coef_hidden = sigma_scale / math.sqrt(F * T)
    has_left, has_right = me > 0, me < T - 1
    has_prev, has_next = s > 0, s < S - 1
    stream = J - keep

    def gu_copies(j, slot):
        cols = pl.ds(pl.multiple_of(j * HB, HB), HB)
        return (
            pltpu.make_async_copy(wg_hbm.at[:, cols], wg.at[slot], w_sem.at[slot, 0]),
            pltpu.make_async_copy(wu_hbm.at[:, cols], wu.at[slot], w_sem.at[slot, 1]),
        )

    def wd_copy(b, slot):
        cols = pl.ds(pl.multiple_of(b * DB, DB), DB)
        return pltpu.make_async_copy(wd_hbm.at[:, cols], wd.at[slot], wd_sem.at[slot])

    def start(copies):
        for copy in copies:
            copy.start()

    def own_copy(c, b):
        cols = pl.ds(pl.multiple_of(b * DB, DB), DB)
        return pltpu.make_async_copy(x_hbm.at[c, :, cols], gx.at[c, me, :, cols], hop_recv.at[c, b])

    def each(count, body):
        lax.fori_loop(0, count, lambda i, z: (body(i), z)[1], 0)

    def between(lo, hi, body):
        lax.fori_loop(lo, hi, lambda i, z: (body(i), z)[1], 0)

    @pl.when(s == 0)
    def _():
        each(n, lambda c: each(Nd, lambda b: own_copy(c, b).start()))

    for j in range(keep + ring):
        start(gu_copies(j, j))
    for b in range(dring):
        wd_copy(b, b).start()

    barrier = pltpu.get_barrier_semaphore()

    def greet(cond, device):
        @pl.when(cond)
        def _():
            pl.semaphore_signal(barrier, inc=1, device_id=device, device_id_type=MESH)

    greet(has_left, {"tp": me - 1})
    greet(has_right, {"tp": me + 1})
    greet(has_next, {"pp": s + 1})
    for k in range(1, Pn):
        pl.semaphore_signal(barrier, inc=1, device_id={"pop": lax.rem(p + k, Pn)}, device_id_type=MESH)
    as_int = lambda v: v.astype(jnp.int32)
    pl.semaphore_wait(barrier, as_int(has_left) + as_int(has_right) + as_int(has_prev) + Pn - 1)

    @pl.when(has_prev)
    def _():
        pl.semaphore_signal(ready, inc=1, device_id={"pp": s - 1}, device_id_type=MESH)

    vectors = Exchange((gl, gr, ul, ur, dl, dr, fit), (egl, egr, eul, eur, edl, edr, efit), v_send, v_recv, v_own, p, Pn)

    def side_rows(first, second, target):
        width = target.shape[1]
        stack[...] = jnp.zeros_like(stack)
        stack[0:members, 0:width] = first[...].astype(f32)
        if second is not None:
            stack[members : 2 * members, 0:width] = second[...].astype(f32)
        target[...] = stack[:, 0:width].astype(bf16)

    def ag_copy(c, g, o, right):
        cols = pl.ds(pl.multiple_of(g * GW, GW), GW)
        return pltpu.make_async_remote_copy(
            src_ref=gx.at[c, o, :, cols], dst_ref=gx.at[c, o, :, cols],
            send_sem=(ag_right if right else ag_left).at[c, g, o], recv_sem=ag_recv.at[c, g, o],
            device_id={"tp": me + 1 if right else me - 1}, device_id_type=MESH,
        )

    def ag_send(c, g, o, cond, right):
        @pl.when(cond)
        def _():
            ag_copy(c, g, o, right).start()

    def ag_own(c, g):
        for u in range(GW // DB):
            own_copy(c, g * (GW // DB) + u).wait()
        ag_send(c, g, me, has_right, True)
        ag_send(c, g, me, has_left, False)

    def ag_pass(c, g, k):
        @pl.when(me - k >= 0)
        def _():
            ag_copy(c, g, me - k, True).wait_recv()
            ag_send(c, g, me - k, has_right, True)

        @pl.when(me + k < T)
        def _():
            ag_copy(c, g, me + k, False).wait_recv()
            ag_send(c, g, me + k, has_left, False)

    waves = G + T - 1

    def ag_step(c, w):
        @pl.when(w < G)
        def _():
            ag_own(c, w)

        between(jnp.maximum(1, w - G + 1), jnp.minimum(w, T - 1) + 1, lambda k: ag_pass(c, w - k, k))

    def normalize(c, t):
        total = jnp.zeros((ROWS, 1), f32)
        for b in range(Nd):
            values = gx[c, t, :, b * DB : (b + 1) * DB].astype(f32)
            total = total + jnp.sum(values * values, axis=-1, keepdims=True)
        scale = lax.rsqrt(total / D + norm_eps)
        for b in range(Nd):
            cols = slice(b * DB, (b + 1) * DB)
            values = gx[c, t, :, cols].astype(f32)
            xn[pl.ds(pl.multiple_of(t * ROWS, ROWS), ROWS), cols] = (values * scale * gain[:, cols]).astype(bf16)

    def sum_copy(c, b, k, right):
        buf, blocks = (rr, pl.ds(k + 1, T - 1 - k)) if right else (ll, pl.ds(0, k))
        return pltpu.make_async_remote_copy(
            src_ref=buf.at[c, b, blocks], dst_ref=buf.at[c, b, blocks],
            send_sem=(rr_send if right else ll_send).at[c, b],
            recv_sem=(rr_recv if right else ll_recv).at[c, b],
            device_id={"tp": me + 1 if right else me - 1}, device_id_type=MESH,
        )

    def senders(right):
        return range(T - 1) if right else range(1, T)

    def pass_on(c, b, right):
        buf = rr if right else ll
        for k in senders(right):
            first = k == (0 if right else T - 1)
            lo, hi = (k + 1, T) if right else (0, k)

            @pl.when(me == k)
            def _():
                if first:
                    merge = lambda at: part[b, at]
                else:
                    sum_copy(c, b, k - 1 if right else k + 1, right).wait_recv()
                    merge = lambda at: (buf[c, b, at].astype(f32) + part[b, at].astype(f32)).astype(bf16)
                if T <= 4:
                    for o in range(lo, hi):
                        buf[c, b, o] = merge(o)
                else:

                    def one(o):
                        buf[c, b, o] = merge(o)

                    between(lo, hi, one)
                sum_copy(c, b, k, right).start()

    def hop_copy(c, b):
        cols = pl.ds(pl.multiple_of(b * DB, DB), DB)
        return pltpu.make_async_remote_copy(
            src_ref=xo.at[c, :, cols], dst_ref=gx.at[c, me, :, cols],
            send_sem=hop_send.at[c, b], recv_sem=hop_recv.at[c, b],
            device_id={"pp": s + 1}, device_id_type=MESH,
        )

    def out_copy(c, b):
        cols = pl.ds(pl.multiple_of(b * DB, DB), DB)
        return pltpu.make_async_copy(xo.at[c, :, cols], out_hbm.at[c, :, cols], out_sem.at[c, b])

    def finish(c, b):
        cols = pl.ds(pl.multiple_of(b * DB, DB), DB)
        acc[...] = part[b, me].astype(f32)
        if T > 1:

            @pl.when(me == T - 1)
            def _():
                sum_copy(c, b, T - 2, True).wait_recv()

            @pl.when(me == 0)
            def _():
                sum_copy(c, b, 1, False).wait_recv()

        @pl.when(has_left)
        def _():
            acc[...] += rr[c, b, me].astype(f32)

        @pl.when(has_right)
        def _():
            acc[...] += ll[c, b, me].astype(f32)

        xo[c, :, cols] = (gx[c, me, :, cols].astype(f32) + acc[...]).astype(bf16)
        out_copy(c, b).start()

        @pl.when(has_next)
        def _():
            hop_copy(c, b).start()

    last_hop = jnp.maximum(me, T - 1 - me)

    def rs_step(c, i):
        def at(lag, body):
            b = i - lag * HOP_TICKS

            @pl.when(jnp.logical_and(b >= 0, b < Nd))
            def _():
                body(b)

        at(me, lambda b: pass_on(c, b, True))
        at(T - 1 - me, lambda b: pass_on(c, b, False))
        at(last_hop, lambda b: finish(c, b))

    rs_steps = Nd + (T - 1) * HOP_TICKS
    pair = 2 if J % 2 == 0 else 1
    groups = J // pair
    spill = -(-(rs_steps - Nd) // groups)

    ticks = groups + Nd
    begin = jnp.where(s == 0, FIRST_BEGIN, LATER_BEGIN)

    def gathered(tick):
        done = jnp.clip((tick - begin + GATHER_TICKS) // GATHER_TICKS, 0, waves)
        return jnp.where(tick >= ticks - 1, waves, done)

    def communicate(c, tick):
        @pl.when(c + 1 < n)
        def _():
            lo = jnp.where(tick == 0, 0, gathered(tick - 1))
            between(lo, gathered(tick), lambda k: ag_step(c + 1, k))

    def member_side(sides, first):
        member = lax.broadcasted_iota(jnp.int32, sides.shape, 0) % members + first
        column = lax.broadcasted_iota(jnp.int32, sides.shape, 1)
        return jnp.sum(jnp.where(member == column, sides, 0.0), axis=1, keepdims=True)

    def add_side(product, side, right, cols):
        wide = product.reshape(T, ROWS, product.shape[-1])
        values = right[:, cols].astype(f32)
        member = lax.broadcasted_iota(jnp.int32, (ROWS, values.shape[1]), 0) % members
        rows_of = jnp.zeros((ROWS, values.shape[1]), f32)
        for m in range(members):
            rows_of = jnp.where(member == m, values[m : m + 1], rows_of)
        wide = wide + side[...].reshape(T, ROWS, 1) * rows_of[None]
        return wide.reshape(product.shape)

    NT = (((1,), (1,)), ((), ()))

    side_rows(gl, ul, lefts)
    side_rows(dl, None, downs)
    each(waves, lambda w: ag_step(0, w))

    @pl.when(has_next)
    def _():
        vectors.start()

    def chunk(c):
        each(T, lambda t: normalize(c, t))
        rows = lambda: xn[...]
        sides = coef_in * lax.dot_general(rows(), lefts[...], NT, preferred_element_type=f32)
        side_g[...] = member_side(sides, 0)
        side_u[...] = member_side(sides, members)

        def gu_half(j):
            if stream:
                q = c * stream + j - keep
                slot = jnp.where(j < keep, j, keep + (q + ring) % ring)
            else:
                q, slot = 0, j

            @pl.when(jnp.logical_or(c == 0, j >= keep))
            def _():
                for copy in gu_copies(j, slot):
                    copy.wait()

            cols = pl.ds(pl.multiple_of(j * HB, HB), HB)
            x = rows()
            gate = jnp.dot(x, wg[slot], preferred_element_type=f32)
            upper = jnp.dot(x, wu[slot], preferred_element_type=f32)
            gate = add_side(gate, side_g, gr, cols)
            upper = add_side(upper, side_u, ur, cols)
            hid[:, cols] = (gate / (1.0 + jnp.exp(-gate)) * upper).astype(bf16)
            return q, slot

        def refill(j, q, slot):
            if stream:
                ahead = q + ring

                @pl.when(jnp.logical_and(j >= keep, ahead < n * stream))
                def _():
                    start(gu_copies(keep + ahead % stream, slot))

        def gu(g):
            for u in range(pair):
                j = g * pair + u
                refill(j, *gu_half(j))

            @pl.when(c > 0)
            def _():
                between(Nd + g * spill, jnp.minimum(Nd + (g + 1) * spill, rs_steps), lambda i: rs_step(c - 1, i))

            communicate(c, g)

        each(groups, gu)

        @pl.when(jnp.logical_and(c == 0, has_next))
        def _():
            pl.semaphore_wait(ready, 1)

        side_d[...] = member_side(coef_hidden * lax.dot_general(hid[...], downs[...], NT, preferred_element_type=f32), 0)

        def down(b):
            q = c * Nd + b
            slot = q % dring
            cols = pl.ds(pl.multiple_of(b * DB, DB), DB)
            wd_copy(b, slot).wait()
            term = jnp.dot(hid[...], wd[slot], preferred_element_type=f32)
            part[b] = add_side(term, side_d, dr, cols).astype(bf16).reshape(T, ROWS, DB)

            @pl.when(q + dring < n * Nd)
            def _():
                wd_copy((b + dring) % Nd, slot).start()

            rs_step(c, b)
            communicate(c, groups + b)

        each(Nd, down)

    each(n, chunk)
    between(Nd, rs_steps, lambda i: rs_step(n - 1, i))

    @pl.when(has_next)
    def _():
        vectors.wait()

    def drain(c):
        def gather(g):
            for o in range(T):

                @pl.when(jnp.logical_and(has_right, o <= me))
                def _():
                    ag_copy(c, g, o, True).wait_send()

                @pl.when(jnp.logical_and(has_left, o >= me))
                def _():
                    ag_copy(c, g, o, False).wait_send()

        each(G, gather)

        def block(b):
            for right in (True, False):
                for k in senders(right):

                    @pl.when(me == k)
                    def _():
                        sum_copy(c, b, k, right).wait_send()

            out_copy(c, b).wait()

            @pl.when(has_next)
            def _():
                hop_copy(c, b).wait_send()

        each(Nd, block)

    each(n, drain)


class Exchange:

    def __init__(self, sources, targets, send, recv, own, p, count):
        self.copies = []
        for a, (source, target) in enumerate(zip(sources, targets)):
            self.copies.append(pltpu.make_async_copy(source, target.at[p], own.at[a]))
            for k in range(1, count):
                self.copies.append(
                    pltpu.make_async_remote_copy(
                        src_ref=source, dst_ref=target.at[p], send_sem=send.at[a, k - 1], recv_sem=recv.at[a, k - 1],
                        device_id={"pop": lax.rem(p + k, count)}, device_id_type=MESH,
                    )
                )

    def start(self):
        for copy in self.copies:
            copy.start()

    def wait(self):
        for copy in self.copies:
            copy.wait()


def gather_kernel(Pn, S, *refs):
    sources, targets, (send, recv, own) = refs[:7], refs[7:14], refs[14:]
    p = lax.axis_index("pop")

    @pl.when(lax.axis_index("pp") == S - 1)
    def _():
        barrier = pltpu.get_barrier_semaphore()
        for k in range(1, Pn):
            pl.semaphore_signal(barrier, inc=1, device_id={"pop": lax.rem(p + k, Pn)}, device_id_type=MESH)
        pl.semaphore_wait(barrier, Pn - 1)
        exchange = Exchange(sources, targets, send, recv, own, p, Pn)
        exchange.start()
        exchange.wait()


def updates_kernel(dims, *refs):
    Pn, members, share, D, F, block, last, aliased = dims
    gl, gr, ul, ur, dl, dr, fit = refs[:7]
    refs = refs[7 + aliased :]
    (out_gate, out_up, out_down), refs = refs[:3], refs[3:]
    if not aliased:
        refs[0][...] = jnp.zeros_like(refs[0])
        refs = refs[1:]
    left, right, weights, wide, tall, sem = refs
    population = members * Pn
    p, S = lax.axis_index("pop"), lax.axis_size("pp")
    here = lax.axis_index("pp")

    def spread(source, target, row, scaled):
        for k in range(Pn):
            at = slice(row + k * members, row + (k + 1) * members)
            values = source[k].astype(f32)
            target[at, 0 : values.shape[1]] = values * fit[k][:, :1] if scaled else values

    def product(source_left, source_right, out, stage, rows_total, row_first, col_first):
        columns = stage.shape[2]
        spread(source_left, left, 0, True)
        spread(source_right, right, 0, False)
        values = left[0:population]
        high = values.astype(bf16).astype(f32)
        left[0:population] = high
        left[population : 2 * population] = values - high
        right[population : 2 * population] = right[0:population]
        width = next(w for w in (512, 256, 128) if columns % w == 0)
        for j in range(0, columns, width):
            cols = pl.ds(pl.multiple_of(col_first + j, 128), width)
            weights[:, j : j + width] = right[:, cols].astype(bf16)
        count = rows_total // block

        def put(t, slot):
            rows = pl.ds(pl.multiple_of(t * block, block), block)
            return pltpu.make_async_copy(stage.at[slot], out.at[rows], sem.at[slot])

        def tile(t, z):
            slot = t % 2

            @pl.when(t >= 2)
            def _():
                put(t - 2, slot).wait()

            rows = pl.ds(pl.multiple_of(row_first + t * block, 128), block)
            lhs = left[:, rows].T.astype(bf16)
            for j in range(0, columns, width):
                got = jnp.dot(lhs, weights[:, j : j + width], preferred_element_type=f32)
                stage[slot, :, j : j + width] = got.astype(bf16)
            put(t, slot).start()
            return z

        lax.fori_loop(0, count, tile, 0)
        for t in range(max(0, count - 2), count):
            put(t, t % 2).wait()

    @pl.when(here == S - 1 if last else here < S - 1)
    def _():
        product(gl, gr, out_gate, wide, share, p * share, 0)
        product(ul, ur, out_up, wide, share, p * share, 0)
        product(dl, dr, out_down, tall, F, 0, p * share)


def gather(vectors):
    Pn, S = lax.axis_size("pop"), lax.axis_size("pp")
    dma = pltpu.SemaphoreType.DMA
    vmem, hbm = pl.BlockSpec(memory_space=pltpu.VMEM), pl.BlockSpec(memory_space=pl.ANY)
    return pl.pallas_call(
        functools.partial(gather_kernel, Pn, S),
        out_shape=tuple(jax.ShapeDtypeStruct((Pn,) + v.shape, v.dtype) for v in vectors),
        in_specs=[vmem] * 7,
        out_specs=(hbm,) * 7,
        scratch_shapes=[dma((7, max(1, Pn - 1))), dma((7, max(1, Pn - 1))), dma((7,))],
        compiler_params=pltpu.CompilerParams(collective_id=1, has_side_effects=True),
    )(*vectors)


def updates(everyone, before, after):
    Pn, members, D = everyone[0].shape
    F = everyone[1].shape[2]
    share = D // Pn
    block = next(w for w in (256, 128) if share % w == 0 and F % w == 0)
    last = before is None
    extra = [] if last else list(before) + [after]
    vmem, hbm = pl.BlockSpec(memory_space=pltpu.VMEM), pl.BlockSpec(memory_space=pl.ANY)
    shapes = [(share, F), (share, F), (F, share)]
    rows = 2 * members * Pn
    return pl.pallas_call(
        functools.partial(updates_kernel, (Pn, members, share, D, F, block, last, len(extra))),
        out_shape=tuple(jax.ShapeDtypeStruct(v, bf16) for v in shapes)
        + ((jax.ShapeDtypeStruct((8, 128), f32),) if last else ()),
        in_specs=[vmem] * 7 + [hbm] * len(extra),
        out_specs=(hbm,) * 3 + ((vmem,) if last else ()),
        input_output_aliases={} if last else {7: 0, 8: 1, 9: 2},
        scratch_shapes=[
            pltpu.VMEM((rows, max(D, F)), f32),
            pltpu.VMEM((rows, max(D, F)), f32),
            pltpu.VMEM((rows, max(F, share)), bf16),
            pltpu.VMEM((2, block, F), bf16),
            pltpu.VMEM((2, block, share), bf16),
            pltpu.SemaphoreType.DMA((2,)),
        ],
        compiler_params=pltpu.CompilerParams(has_side_effects=True),
    )(*everyone, *extra)


def relay(x, w_gate, w_up, w_down, gain, vectors, token):
    n, _, D = x.shape
    F = w_gate.shape[1]
    members = vectors[0].shape[0]
    T, S, Pn = (lax.axis_size(a) for a in ("tp", "pp", "pop"))
    HB, DB = widths(D, F)
    J, Nd, M = F // HB, D // DB, T * ROWS
    G = Nd // 2 if Nd % 2 == 0 else Nd
    dring = min(3, Nd)
    side = -(-2 * members // 16) * 16
    fixed = 2 * (n * ROWS * D + M * D + n * M * D + M * F + M * D + 2 * n * M * D + dring * F * DB + 4 * side * max(D, F)) + RESERVE
    slots = min(J, (VMEM_BYTES - fixed) // (4 * D * HB))
    ring = 0 if slots == J else min(3, slots)
    keep = slots - ring
    dims = (n, T, S, Pn, members, D, F, HB, DB, keep, ring, dring)
    vmem, hbm = pl.BlockSpec(memory_space=pltpu.VMEM), pl.BlockSpec(memory_space=pl.ANY)
    dma = pltpu.SemaphoreType.DMA
    return pl.pallas_call(
        functools.partial(relay_kernel, dims),
        out_shape=(jax.ShapeDtypeStruct((n, ROWS, D), bf16),)
        + tuple(jax.ShapeDtypeStruct((Pn,) + v.shape, v.dtype) for v in vectors),
        in_specs=[hbm] * 4 + [vmem] * 9,
        out_specs=(hbm,) * 8,
        scratch_shapes=[
            pltpu.VMEM((n, T, ROWS, D), bf16),
            pltpu.VMEM((M, D), bf16),
            pltpu.VMEM((M, F), bf16),
            pltpu.VMEM((Nd, T, ROWS, DB), bf16),
            pltpu.VMEM((n, Nd, T, ROWS, DB), bf16),
            pltpu.VMEM((n, Nd, T, ROWS, DB), bf16),
            pltpu.VMEM((n, ROWS, D), bf16),
            pltpu.VMEM((ROWS, DB), f32),
            pltpu.VMEM((M, 1), f32),
            pltpu.VMEM((M, 1), f32),
            pltpu.VMEM((M, 1), f32),
            pltpu.VMEM((slots, D, HB), bf16),
            pltpu.VMEM((slots, D, HB), bf16),
            pltpu.VMEM((dring, F, DB), bf16),
            pltpu.VMEM((side, max(D, F)), f32),
            pltpu.VMEM((side, D), bf16),
            pltpu.VMEM((side, F), bf16),
            dma((slots, 2)),
            dma((dring,)),
            dma((n, Nd)),
            dma((n, Nd)),
            dma((n, Nd)),
            dma((n, G, T)),
            dma((n, G, T)),
            dma((n, G, T)),
            dma((n, Nd)),
            dma((n, Nd)),
            dma((n, Nd)),
            dma((n, Nd)),
            dma((7, max(1, Pn - 1))),
            dma((7, max(1, Pn - 1))),
            dma((7,)),
            pltpu.SemaphoreType.REGULAR,
        ],
        compiler_params=pltpu.CompilerParams(collective_id=0, has_side_effects=True, vmem_limit_bytes=67_000_000),
    )(x, w_gate, w_up, w_down, gain, *vectors, token)


def per_device(
    hidden_in, norm_gain, w_gate, w_up, w_down,
    gate_left, gate_right, up_left, up_right, down_left, down_right, ranks,
):
    tokens, members, D = hidden_in.shape
    population = members * lax.axis_size("pop")
    fitness = (2.0 * ranks.astype(f32) / (population - 1) - 1.0) / math.sqrt(population)
    vectors = [gate_left[0], gate_right[0], up_left[0], up_right[0], down_left[0], down_right[0]]
    vectors.append(jnp.broadcast_to(fitness[:, None], (members, 128)))
    *last, token = updates(gather(vectors), None, None)
    x = hidden_in.reshape(tokens * members // ROWS, ROWS, D)
    out, *everyone = relay(x, w_gate[0], w_up[0], w_down[0], norm_gain, vectors, token)
    update_gate, update_up, update_down = updates(everyone, last, out)
    return (out.reshape(1, tokens, members, D), update_gate[None], update_up[None], update_down[None])


def solution(mesh):
    placed = (
        P("tp", "pop", None),
        P("pp", None),
        P("pp", None, "tp"),
        P("pp", None, "tp"),
        P("pp", "tp", None),
        P("pp", "pop", None),
        P("pp", "pop", "tp"),
        P("pp", "pop", None),
        P("pp", "pop", "tp"),
        P("pp", "pop", "tp"),
        P("pp", "pop", None),
        P("pop"),
    )
    return jax.shard_map(
        per_device,
        mesh=mesh,
        in_specs=placed,
        out_specs=(
            P("pp", "tp", "pop", None),
            P("pp", "pop", "tp"),
            P("pp", "pop", "tp"),
            P("pp", "tp", "pop"),
        ),
        check_vma=False,
    )
```

```python
import functools
import math

import jax
import jax.numpy as jnp
from jax import lax
from jax.experimental import pallas as pl
from jax.experimental.pallas import tpu as pltpu
from jax.sharding import PartitionSpec as P

MESH = pl.DeviceIdType.MESH
f32, bf16 = jnp.float32, jnp.bfloat16

sigma_scale = 0.3
norm_eps = 1e-05

ROWS = 32
HOP_TICKS = 4
GATHER_TICKS = 3
FIRST_BEGIN = 0
FIRST_PAUSE = 7
LATER_BEGIN = 1
VMEM_BYTES = 66_000_000
RESERVE = 1_500_000


def widths(D, F):
    hidden = next(w for w in (256, 128) if F % w == 0)
    columns = next(w for w in (512, 256, 128) if D % w == 0 and D // w >= 4)
    return hidden, columns


def relay_kernel(
    dims,
    x_hbm, wg_hbm, wu_hbm, wd_hbm, gain, gl, gr, ul, ur, dl, dr, fit, token,
    out_hbm, egl, egr, eul, eur, edl, edr, efit,
    gx, xn, hid, part, rr, ll, xo, acc, side_g, side_u, side_d, wg, wu, wd, stack, lefts, downs,
    w_sem, wd_sem, hop_recv, hop_send, out_sem,
    ag_recv, ag_right, ag_left, rr_recv, rr_send, ll_recv, ll_send,
    v_send, v_recv, v_own, ready,
):
    n, T, S, Pn, members, D, F, HB, DB, keep, ring, dring = dims
    J, Nd, M = F // HB, D // DB, T * ROWS
    G = Nd // 2 if Nd % 2 == 0 else Nd
    GW = D // G
    me, s, p = lax.axis_index("tp"), lax.axis_index("pp"), lax.axis_index("pop")
    coef_in = sigma_scale / math.sqrt(D)
    coef_hidden = sigma_scale / math.sqrt(F * T)
    has_left, has_right = me > 0, me < T - 1
    has_prev, has_next = s > 0, s < S - 1
    stream = J - keep

    def gu_copies(j, slot):
        cols = pl.ds(pl.multiple_of(j * HB, HB), HB)
        return (
            pltpu.make_async_copy(wg_hbm.at[:, cols], wg.at[slot], w_sem.at[slot, 0]),
            pltpu.make_async_copy(wu_hbm.at[:, cols], wu.at[slot], w_sem.at[slot, 1]),
        )

    def wd_copy(b, slot):
        cols = pl.ds(pl.multiple_of(b * DB, DB), DB)
        return pltpu.make_async_copy(wd_hbm.at[:, cols], wd.at[slot], wd_sem.at[slot])

    def start(copies):
        for copy in copies:
            copy.start()

    def own_copy(c, b):
        cols = pl.ds(pl.multiple_of(b * DB, DB), DB)
        return pltpu.make_async_copy(x_hbm.at[c, :, cols], gx.at[c, me, :, cols], hop_recv.at[c, b])

    def each(count, body):
        lax.fori_loop(0, count, lambda i, z: (body(i), z)[1], 0)

    def between(lo, hi, body):
        lax.fori_loop(lo, hi, lambda i, z: (body(i), z)[1], 0)

    @pl.when(s == 0)
    def _():
        each(n, lambda c: each(Nd, lambda b: own_copy(c, b).start()))

    for j in range(keep + ring):
        start(gu_copies(j, j))
    for b in range(dring):
        wd_copy(b, b).start()

    barrier = pltpu.get_barrier_semaphore()

    def greet(cond, device):
        @pl.when(cond)
        def _():
            pl.semaphore_signal(barrier, inc=1, device_id=device, device_id_type=MESH)

    greet(has_left, {"tp": me - 1})
    greet(has_right, {"tp": me + 1})
    greet(has_next, {"pp": s + 1})
    for k in range(1, Pn):
        pl.semaphore_signal(barrier, inc=1, device_id={"pop": lax.rem(p + k, Pn)}, device_id_type=MESH)
    as_int = lambda v: v.astype(jnp.int32)
    pl.semaphore_wait(barrier, as_int(has_left) + as_int(has_right) + as_int(has_prev) + Pn - 1)

    @pl.when(has_prev)
    def _():
        pl.semaphore_signal(ready, inc=1, device_id={"pp": s - 1}, device_id_type=MESH)

    vectors = Exchange((gl, gr, ul, ur, dl, dr, fit), (egl, egr, eul, eur, edl, edr, efit), v_send, v_recv, v_own, p, Pn)

    def side_rows(first, second, target):
        width = target.shape[1]
        stack[...] = jnp.zeros_like(stack)
        stack[0:members, 0:width] = first[...].astype(f32)
        if second is not None:
            stack[members : 2 * members, 0:width] = second[...].astype(f32)
        target[...] = stack[:, 0:width].astype(bf16)

    def ag_copy(c, g, o, right):
        cols = pl.ds(pl.multiple_of(g * GW, GW), GW)
        return pltpu.make_async_remote_copy(
            src_ref=gx.at[c, o, :, cols], dst_ref=gx.at[c, o, :, cols],
            send_sem=(ag_right if right else ag_left).at[c, g, o], recv_sem=ag_recv.at[c, g, o],
            device_id={"tp": me + 1 if right else me - 1}, device_id_type=MESH,
        )

    def ag_send(c, g, o, cond, right):
        @pl.when(cond)
        def _():
            ag_copy(c, g, o, right).start()

    def ag_own(c, g):
        for u in range(GW // DB):
            own_copy(c, g * (GW // DB) + u).wait()
        ag_send(c, g, me, has_right, True)
        ag_send(c, g, me, has_left, False)

    def ag_pass(c, g, k):
        @pl.when(me - k >= 0)
        def _():
            ag_copy(c, g, me - k, True).wait_recv()
            ag_send(c, g, me - k, has_right, True)

        @pl.when(me + k < T)
        def _():
            ag_copy(c, g, me + k, False).wait_recv()
            ag_send(c, g, me + k, has_left, False)

    steps = jnp.where(s == 0, G * T, G + T - 1)

    def ag_step(c, i):
        @pl.when(s == 0)
        def _():
            k, g = i // G, i % G

            @pl.when(k == 0)
            def _():
                ag_own(c, g)

            @pl.when(k > 0)
            def _():
                ag_pass(c, g, k)

        @pl.when(s > 0)
        def _():
            @pl.when(i < G)
            def _():
                ag_own(c, i)

            between(jnp.maximum(1, i - G + 1), jnp.minimum(i, T - 1) + 1, lambda k: ag_pass(c, i - k, k))

    def normalize(c, t):
        total = jnp.zeros((ROWS, 1), f32)
        for b in range(Nd):
            values = gx[c, t, :, b * DB : (b + 1) * DB].astype(f32)
            total = total + jnp.sum(values * values, axis=-1, keepdims=True)
        scale = lax.rsqrt(total / D + norm_eps)
        for b in range(Nd):
            cols = slice(b * DB, (b + 1) * DB)
            values = gx[c, t, :, cols].astype(f32)
            xn[pl.ds(pl.multiple_of(t * ROWS, ROWS), ROWS), cols] = (values * scale * gain[:, cols]).astype(bf16)

    def sum_copy(c, b, k, right):
        buf, blocks = (rr, pl.ds(k + 1, T - 1 - k)) if right else (ll, pl.ds(0, k))
        return pltpu.make_async_remote_copy(
            src_ref=buf.at[c, b, blocks], dst_ref=buf.at[c, b, blocks],
            send_sem=(rr_send if right else ll_send).at[c, b],
            recv_sem=(rr_recv if right else ll_recv).at[c, b],
            device_id={"tp": me + 1 if right else me - 1}, device_id_type=MESH,
        )

    def senders(right):
        return range(T - 1) if right else range(1, T)

    def pass_on(c, b, right):
        buf = rr if right else ll
        for k in senders(right):
            first = k == (0 if right else T - 1)
            lo, hi = (k + 1, T) if right else (0, k)

            @pl.when(me == k)
            def _():
                if first:
                    merge = lambda at: part[b, at]
                else:
                    sum_copy(c, b, k - 1 if right else k + 1, right).wait_recv()
                    merge = lambda at: (buf[c, b, at].astype(f32) + part[b, at].astype(f32)).astype(bf16)
                if T <= 4:
                    for o in range(lo, hi):
                        buf[c, b, o] = merge(o)
                else:

                    def one(o):
                        buf[c, b, o] = merge(o)

                    between(lo, hi, one)
                sum_copy(c, b, k, right).start()

    def hop_copy(c, b):
        cols = pl.ds(pl.multiple_of(b * DB, DB), DB)
        return pltpu.make_async_remote_copy(
            src_ref=xo.at[c, :, cols], dst_ref=gx.at[c, me, :, cols],
            send_sem=hop_send.at[c, b], recv_sem=hop_recv.at[c, b],
            device_id={"pp": s + 1}, device_id_type=MESH,
        )

    def out_copy(c, b):
        cols = pl.ds(pl.multiple_of(b * DB, DB), DB)
        return pltpu.make_async_copy(xo.at[c, :, cols], out_hbm.at[c, :, cols], out_sem.at[c, b])

    def finish(c, b):
        cols = pl.ds(pl.multiple_of(b * DB, DB), DB)
        acc[...] = part[b, me].astype(f32)
        if T > 1:

            @pl.when(me == T - 1)
            def _():
                sum_copy(c, b, T - 2, True).wait_recv()

            @pl.when(me == 0)
            def _():
                sum_copy(c, b, 1, False).wait_recv()

        @pl.when(has_left)
        def _():
            acc[...] += rr[c, b, me].astype(f32)

        @pl.when(has_right)
        def _():
            acc[...] += ll[c, b, me].astype(f32)

        xo[c, :, cols] = (gx[c, me, :, cols].astype(f32) + acc[...]).astype(bf16)
        out_copy(c, b).start()

        @pl.when(has_next)
        def _():
            hop_copy(c, b).start()

    last_hop = jnp.maximum(me, T - 1 - me)

    def rs_step(c, i):
        def at(lag, body):
            b = i - lag * HOP_TICKS

            @pl.when(jnp.logical_and(b >= 0, b < Nd))
            def _():
                body(b)

        at(me, lambda b: pass_on(c, b, True))
        at(T - 1 - me, lambda b: pass_on(c, b, False))
        at(last_hop, lambda b: finish(c, b))

    rs_steps = Nd + (T - 1) * HOP_TICKS
    pair = 1
    groups = J // pair
    spill = -(-(rs_steps - Nd) // groups)

    ticks = groups + Nd
    begin = jnp.where(s == 0, FIRST_BEGIN, LATER_BEGIN)

    def gathered(tick):
        first = jnp.where(tick < begin, 0, G + (jnp.maximum(tick - begin - FIRST_PAUSE, 0) * G * (T - 1)) // max(1, ticks - FIRST_PAUSE - 2))
        later = (tick - begin + GATHER_TICKS) // GATHER_TICKS
        done = jnp.clip(jnp.where(s == 0, first, later), 0, steps)
        return jnp.where(tick >= ticks - 1, steps, done)

    def communicate(c, tick):
        @pl.when(c + 1 < n)
        def _():
            lo = jnp.where(tick == 0, 0, gathered(tick - 1))
            between(lo, gathered(tick), lambda k: ag_step(c + 1, k))

    def member_side(sides, first):
        member = lax.broadcasted_iota(jnp.int32, sides.shape, 0) % members + first
        column = lax.broadcasted_iota(jnp.int32, sides.shape, 1)
        return jnp.sum(jnp.where(member == column, sides, 0.0), axis=1, keepdims=True)

    def add_side(product, side, right, cols):
        wide = product.reshape(T, ROWS, product.shape[-1])
        values = right[:, cols].astype(f32)
        member = lax.broadcasted_iota(jnp.int32, (ROWS, values.shape[1]), 0) % members
        rows_of = jnp.zeros((ROWS, values.shape[1]), f32)
        for m in range(members):
            rows_of = jnp.where(member == m, values[m : m + 1], rows_of)
        wide = wide + side[...].reshape(T, ROWS, 1) * rows_of[None]
        return wide.reshape(product.shape)

    NT = (((1,), (1,)), ((), ()))

    side_rows(gl, ul, lefts)
    side_rows(dl, None, downs)
    each(steps, lambda i: ag_step(0, i))

    @pl.when(has_next)
    def _():
        vectors.start()

    def chunk(c):
        each(T, lambda t: normalize(c, t))
        rows = lambda: xn[...]
        sides = coef_in * lax.dot_general(rows(), lefts[...], NT, preferred_element_type=f32)
        side_g[...] = member_side(sides, 0)
        side_u[...] = member_side(sides, members)

        def gu_half(j):
            if stream:
                q = c * stream + j - keep
                slot = jnp.where(j < keep, j, keep + (q + ring) % ring)
            else:
                q, slot = 0, j

            @pl.when(jnp.logical_or(c == 0, j >= keep))
            def _():
                for copy in gu_copies(j, slot):
                    copy.wait()

            cols = pl.ds(pl.multiple_of(j * HB, HB), HB)
            x = rows()
            gate = jnp.dot(x, wg[slot], preferred_element_type=f32)
            upper = jnp.dot(x, wu[slot], preferred_element_type=f32)
            gate = add_side(gate, side_g, gr, cols)
            upper = add_side(upper, side_u, ur, cols)
            hid[:, cols] = (gate / (1.0 + jnp.exp(-gate)) * upper).astype(bf16)
            return q, slot

        def refill(j, q, slot):
            if stream:
                ahead = q + ring

                @pl.when(jnp.logical_and(j >= keep, ahead < n * stream))
                def _():
                    start(gu_copies(keep + ahead % stream, slot))

        def gu(g):
            for u in range(pair):
                j = g * pair + u
                refill(j, *gu_half(j))

            @pl.when(c > 0)
            def _():
                between(Nd + g * spill, jnp.minimum(Nd + (g + 1) * spill, rs_steps), lambda i: rs_step(c - 1, i))

            communicate(c, g)

        each(groups, gu)

        @pl.when(jnp.logical_and(c == 0, has_next))
        def _():
            pl.semaphore_wait(ready, 1)

        side_d[...] = member_side(coef_hidden * lax.dot_general(hid[...], downs[...], NT, preferred_element_type=f32), 0)

        def down(b):
            q = c * Nd + b
            slot = q % dring
            cols = pl.ds(pl.multiple_of(b * DB, DB), DB)
            wd_copy(b, slot).wait()
            term = jnp.dot(hid[...], wd[slot], preferred_element_type=f32)
            part[b] = add_side(term, side_d, dr, cols).astype(bf16).reshape(T, ROWS, DB)

            @pl.when(q + dring < n * Nd)
            def _():
                wd_copy((b + dring) % Nd, slot).start()

            rs_step(c, b)
            communicate(c, groups + b)

        each(Nd, down)

    each(n, chunk)
    between(Nd, rs_steps, lambda i: rs_step(n - 1, i))

    @pl.when(has_next)
    def _():
        vectors.wait()

    def drain(c):
        def gather(g):
            for o in range(T):

                @pl.when(jnp.logical_and(has_right, o <= me))
                def _():
                    ag_copy(c, g, o, True).wait_send()

                @pl.when(jnp.logical_and(has_left, o >= me))
                def _():
                    ag_copy(c, g, o, False).wait_send()

        each(G, gather)

        def block(b):
            for right in (True, False):
                for k in senders(right):

                    @pl.when(me == k)
                    def _():
                        sum_copy(c, b, k, right).wait_send()

            out_copy(c, b).wait()

            @pl.when(has_next)
            def _():
                hop_copy(c, b).wait_send()

        each(Nd, block)

    each(n, drain)


class Exchange:

    def __init__(self, sources, targets, send, recv, own, p, count):
        self.copies = []
        for a, (source, target) in enumerate(zip(sources, targets)):
            self.copies.append(pltpu.make_async_copy(source, target.at[p], own.at[a]))
            for k in range(1, count):
                self.copies.append(
                    pltpu.make_async_remote_copy(
                        src_ref=source, dst_ref=target.at[p], send_sem=send.at[a, k - 1], recv_sem=recv.at[a, k - 1],
                        device_id={"pop": lax.rem(p + k, count)}, device_id_type=MESH,
                    )
                )

    def start(self):
        for copy in self.copies:
            copy.start()

    def wait(self):
        for copy in self.copies:
            copy.wait()


def gather_kernel(Pn, S, *refs):
    sources, targets, (send, recv, own) = refs[:7], refs[7:14], refs[14:]
    p = lax.axis_index("pop")

    @pl.when(lax.axis_index("pp") == S - 1)
    def _():
        barrier = pltpu.get_barrier_semaphore()
        for k in range(1, Pn):
            pl.semaphore_signal(barrier, inc=1, device_id={"pop": lax.rem(p + k, Pn)}, device_id_type=MESH)
        pl.semaphore_wait(barrier, Pn - 1)
        exchange = Exchange(sources, targets, send, recv, own, p, Pn)
        exchange.start()
        exchange.wait()


def updates_kernel(dims, *refs):
    Pn, members, share, D, F, block, last, aliased = dims
    gl, gr, ul, ur, dl, dr, fit = refs[:7]
    refs = refs[7 + aliased :]
    (out_gate, out_up, out_down), refs = refs[:3], refs[3:]
    if not aliased:
        refs[0][...] = jnp.zeros_like(refs[0])
        refs = refs[1:]
    left, right, weights, wide, tall, sem = refs
    population = members * Pn
    p, S = lax.axis_index("pop"), lax.axis_size("pp")
    here = lax.axis_index("pp")

    def spread(source, target, row, scaled):
        for k in range(Pn):
            at = slice(row + k * members, row + (k + 1) * members)
            values = source[k].astype(f32)
            target[at, 0 : values.shape[1]] = values * fit[k][:, :1] if scaled else values

    def product(source_left, source_right, out, stage, rows_total, row_first, col_first):
        columns = stage.shape[2]
        spread(source_left, left, 0, True)
        spread(source_right, right, 0, False)
        values = left[0:population]
        high = values.astype(bf16).astype(f32)
        left[0:population] = high
        left[population : 2 * population] = values - high
        right[population : 2 * population] = right[0:population]
        width = next(w for w in (512, 256, 128) if columns % w == 0)
        for j in range(0, columns, width):
            cols = pl.ds(pl.multiple_of(col_first + j, 128), width)
            weights[:, j : j + width] = right[:, cols].astype(bf16)
        count = rows_total // block

        def put(t, slot):
            rows = pl.ds(pl.multiple_of(t * block, block), block)
            return pltpu.make_async_copy(stage.at[slot], out.at[rows], sem.at[slot])

        def tile(t, z):
            slot = t % 2

            @pl.when(t >= 2)
            def _():
                put(t - 2, slot).wait()

            rows = pl.ds(pl.multiple_of(row_first + t * block, 128), block)
            lhs = left[:, rows].T.astype(bf16)
            for j in range(0, columns, width):
                got = jnp.dot(lhs, weights[:, j : j + width], preferred_element_type=f32)
                stage[slot, :, j : j + width] = got.astype(bf16)
            put(t, slot).start()
            return z

        lax.fori_loop(0, count, tile, 0)
        for t in range(max(0, count - 2), count):
            put(t, t % 2).wait()

    @pl.when(here == S - 1 if last else here < S - 1)
    def _():
        product(gl, gr, out_gate, wide, share, p * share, 0)
        product(ul, ur, out_up, wide, share, p * share, 0)
        product(dl, dr, out_down, tall, F, 0, p * share)


def gather(vectors):
    Pn, S = lax.axis_size("pop"), lax.axis_size("pp")
    dma = pltpu.SemaphoreType.DMA
    vmem, hbm = pl.BlockSpec(memory_space=pltpu.VMEM), pl.BlockSpec(memory_space=pl.ANY)
    return pl.pallas_call(
        functools.partial(gather_kernel, Pn, S),
        out_shape=tuple(jax.ShapeDtypeStruct((Pn,) + v.shape, v.dtype) for v in vectors),
        in_specs=[vmem] * 7,
        out_specs=(hbm,) * 7,
        scratch_shapes=[dma((7, max(1, Pn - 1))), dma((7, max(1, Pn - 1))), dma((7,))],
        compiler_params=pltpu.CompilerParams(collective_id=1, has_side_effects=True),
    )(*vectors)


def updates(everyone, before, after):
    Pn, members, D = everyone[0].shape
    F = everyone[1].shape[2]
    share = D // Pn
    block = next(w for w in (256, 128) if share % w == 0 and F % w == 0)
    last = before is None
    extra = [] if last else list(before) + [after]
    vmem, hbm = pl.BlockSpec(memory_space=pltpu.VMEM), pl.BlockSpec(memory_space=pl.ANY)
    shapes = [(share, F), (share, F), (F, share)]
    rows = 2 * members * Pn
    return pl.pallas_call(
        functools.partial(updates_kernel, (Pn, members, share, D, F, block, last, len(extra))),
        out_shape=tuple(jax.ShapeDtypeStruct(v, bf16) for v in shapes)
        + ((jax.ShapeDtypeStruct((8, 128), f32),) if last else ()),
        in_specs=[vmem] * 7 + [hbm] * len(extra),
        out_specs=(hbm,) * 3 + ((vmem,) if last else ()),
        input_output_aliases={} if last else {7: 0, 8: 1, 9: 2},
        scratch_shapes=[
            pltpu.VMEM((rows, max(D, F)), f32),
            pltpu.VMEM((rows, max(D, F)), f32),
            pltpu.VMEM((rows, max(F, share)), bf16),
            pltpu.VMEM((2, block, F), bf16),
            pltpu.VMEM((2, block, share), bf16),
            pltpu.SemaphoreType.DMA((2,)),
        ],
        compiler_params=pltpu.CompilerParams(has_side_effects=True),
    )(*everyone, *extra)


def relay(x, w_gate, w_up, w_down, gain, vectors, token):
    n, _, D = x.shape
    F = w_gate.shape[1]
    members = vectors[0].shape[0]
    T, S, Pn = (lax.axis_size(a) for a in ("tp", "pp", "pop"))
    HB, DB = widths(D, F)
    J, Nd, M = F // HB, D // DB, T * ROWS
    G = Nd // 2 if Nd % 2 == 0 else Nd
    dring = min(3, Nd)
    side = -(-2 * members // 16) * 16
    fixed = 2 * (n * ROWS * D + M * D + n * M * D + M * F + M * D + 2 * n * M * D + dring * F * DB + 4 * side * max(D, F)) + RESERVE
    slots = min(J, (VMEM_BYTES - fixed) // (4 * D * HB))
    ring = 0 if slots == J else min(3, slots)
    keep = slots - ring
    dims = (n, T, S, Pn, members, D, F, HB, DB, keep, ring, dring)
    vmem, hbm = pl.BlockSpec(memory_space=pltpu.VMEM), pl.BlockSpec(memory_space=pl.ANY)
    dma = pltpu.SemaphoreType.DMA
    return pl.pallas_call(
        functools.partial(relay_kernel, dims),
        out_shape=(jax.ShapeDtypeStruct((n, ROWS, D), bf16),)
        + tuple(jax.ShapeDtypeStruct((Pn,) + v.shape, v.dtype) for v in vectors),
        in_specs=[hbm] * 4 + [vmem] * 9,
        out_specs=(hbm,) * 8,
        scratch_shapes=[
            pltpu.VMEM((n, T, ROWS, D), bf16),
            pltpu.VMEM((M, D), bf16),
            pltpu.VMEM((M, F), bf16),
            pltpu.VMEM((Nd, T, ROWS, DB), bf16),
            pltpu.VMEM((n, Nd, T, ROWS, DB), bf16),
            pltpu.VMEM((n, Nd, T, ROWS, DB), bf16),
            pltpu.VMEM((n, ROWS, D), bf16),
            pltpu.VMEM((ROWS, DB), f32),
            pltpu.VMEM((M, 1), f32),
            pltpu.VMEM((M, 1), f32),
            pltpu.VMEM((M, 1), f32),
            pltpu.VMEM((slots, D, HB), bf16),
            pltpu.VMEM((slots, D, HB), bf16),
            pltpu.VMEM((dring, F, DB), bf16),
            pltpu.VMEM((side, max(D, F)), f32),
            pltpu.VMEM((side, D), bf16),
            pltpu.VMEM((side, F), bf16),
            dma((slots, 2)),
            dma((dring,)),
            dma((n, Nd)),
            dma((n, Nd)),
            dma((n, Nd)),
            dma((n, G, T)),
            dma((n, G, T)),
            dma((n, G, T)),
            dma((n, Nd)),
            dma((n, Nd)),
            dma((n, Nd)),
            dma((n, Nd)),
            dma((7, max(1, Pn - 1))),
            dma((7, max(1, Pn - 1))),
            dma((7,)),
            pltpu.SemaphoreType.REGULAR,
        ],
        compiler_params=pltpu.CompilerParams(collective_id=0, has_side_effects=True, vmem_limit_bytes=67_000_000),
    )(x, w_gate, w_up, w_down, gain, *vectors, token)


def per_device(
    hidden_in, norm_gain, w_gate, w_up, w_down,
    gate_left, gate_right, up_left, up_right, down_left, down_right, ranks,
):
    tokens, members, D = hidden_in.shape
    population = members * lax.axis_size("pop")
    fitness = (2.0 * ranks.astype(f32) / (population - 1) - 1.0) / math.sqrt(population)
    vectors = [gate_left[0], gate_right[0], up_left[0], up_right[0], down_left[0], down_right[0]]
    vectors.append(jnp.broadcast_to(fitness[:, None], (members, 128)))
    *last, token = updates(gather(vectors), None, None)
    x = hidden_in.reshape(tokens * members // ROWS, ROWS, D)
    out, *everyone = relay(x, w_gate[0], w_up[0], w_down[0], norm_gain, vectors, token)
    update_gate, update_up, update_down = updates(everyone, last, out)
    return (out.reshape(1, tokens, members, D), update_gate[None], update_up[None], update_down[None])


def solution(mesh):
    placed = (
        P("tp", "pop", None),
        P("pp", None),
        P("pp", None, "tp"),
        P("pp", None, "tp"),
        P("pp", "tp", None),
        P("pp", "pop", None),
        P("pp", "pop", "tp"),
        P("pp", "pop", None),
        P("pp", "pop", "tp"),
        P("pp", "pop", "tp"),
        P("pp", "pop", None),
        P("pop"),
    )
    return jax.shard_map(
        per_device,
        mesh=mesh,
        in_specs=placed,
        out_specs=(
            P("pp", "tp", "pop", None),
            P("pp", "pop", "tp"),
            P("pp", "pop", "tp"),
            P("pp", "tp", "pop"),
        ),
        check_vma=False,
    )
```
